512 devices in a mesh: group: 2 (over y), tm: 16 (over z), bl: 8 (over x), pol: 2 (over core).
Axes of the slice: x: 8, y: 2, z: 16, core: 2. Of those that a mesh axis runs over, the one named last changes fastest.
The devices are a block of a 8x8x16 slice.
Arguments:
- visibilities: bfloat16 [6400, 256, 2, 384], P(('group', 'tm'), ('bl', 'pol')), parts along dimension 0, may hold values from -6 to 6
- flag_mask: int32 [6400], P(('group', 'tm')), parts along dimension 0, may hold values 0 or 1
- kernel_index: int32 [256], P(('bl', 'pol')), may hold values from 0 to 15
- filter_bank: float32 [2, 16, 257], replicated, may hold values from -0.875 to 0.875
Outputs:
- fringe_filtered: bfloat16 [640, 256, 2, 384], P('group', ('bl', 'pol', 'tm')), parts along dimension 0
The draws below stay inside these ranges and needn't reach their ends.
There are 2 independent parts, one for each index of `group`. The reference program is written for one: setup_inputs(seed, part) draws one part's arguments, and reference() takes and returns one part's arrays. A program takes and returns all parts, laid end to end along the dimension named above; an argument that names none is the same for every part. Nothing has to cross between parts.
All inputs are finite; a program needn't handle non-finite values. No bound on the sum of `flag_mask` on one device may be relied on, other than what follows from the above.
Results may differ from the reference program's by a relative error of at most 0.001.
Values may be sent and summed in bfloat16 or wider, within the bound.
A program may use at most 128 MiB of HBM per device.

```python
import jax
import jax.numpy as jnp
from jax import lax

BASE = 256
CHAN = 384
TAPS = 257
AVG = 10
NKERN = 16
T_DEV = 200
TIMES = 3200
OUT_TIMES = 320


def place_ends(array, stream_key, least, top_value):
    index_at = [jax.random.randint(jax.random.fold_in(stream_key, axis), (), 0, length) for axis, length in enumerate(array.shape)]
    widest = array.shape.index(max(array.shape))
    neighbour = index_at[:widest] + [(index_at[widest] + 1) % array.shape[widest]] + index_at[widest + 1:]
    return array.at[tuple(index_at)].set(least).at[tuple(neighbour)].set(top_value)


def block_levels(own_key, shape, shards, smallest, largest):
    level, own = 1.0, jax.random.fold_in(own_key, 6)
    for position, shards_of in shards:
        draws = jnp.exp(jax.random.uniform(jax.random.fold_in(own, position), (shards_of,), jnp.float32, smallest / len(shards), largest / len(shards)))
        level = level * jnp.repeat(draws, shape[position] // shards_of).reshape([-1 if axis == position else 1 for axis in range(len(shape))])
    return level


def gaussian(own_key, shape, scale, limit, pieces=(), kind=jnp.bfloat16):
    factor_of = block_levels(own_key, shape, pieces, -0.22, 0.18) if pieces else 1.0
    entries = jax.random.normal(own_key, shape, jnp.float32) * scale * factor_of
    return jnp.minimum(jnp.maximum(entries, -limit), limit).astype(kind)


def setup_inputs(seed: int = 0, part: int = 0) -> dict:
    keys = jax.random.split(jax.random.key(seed), 5)
    part_splits = jax.random.split(jax.random.fold_in(keys[4], part), 5)
    visibilities = gaussian(part_splits[0], (TIMES, BASE, 2, CHAN), 1.0, 6.0, ((0, 16), (1, 16)))
    flag_mask = place_ends((jax.random.randint(part_splits[1], (TIMES,), 0, 10) < 9).astype(jnp.int32), jax.random.fold_in(part_splits[1], 1), 0, 1)
    kernel_index = place_ends(jax.random.randint(keys[2], (BASE,), 0, NKERN), jax.random.fold_in(keys[2], 1), 0, NKERN - 1).astype(jnp.int32)
    filter_bank = gaussian(keys[3], (2, NKERN, TAPS), (TAPS // 5) ** -0.5, 0.875, (), jnp.float32)
    return {"visibilities": visibilities, "flag_mask": flag_mask, "kernel_index": kernel_index, "filter_bank": filter_bank}


def select_taps(kernel_index, filter_bank):
    choices_count = filter_bank.shape[1]
    one_hot = (kernel_index[:, None] == jnp.arange(choices_count, dtype=jnp.int32)[None, :]).astype(jnp.float32)
    return jnp.einsum("bk,rkt->brt", one_hot, filter_bank, precision=lax.Precision.HIGHEST)


def make_band(kernel_taps, block_rows):
    tap_count = kernel_taps.shape[1]
    row_width = block_rows + tap_count - 1
    zero_tail = jnp.zeros((2, block_rows), jnp.float32)
    period_row = jnp.concatenate([kernel_taps, zero_tail], axis=1)
    tiled_rows = jnp.tile(period_row, (1, block_rows))[:, :block_rows * row_width]
    return tiled_rows.reshape(2, block_rows, row_width)


def filter_block(time_slab, kernel_taps, block_rows, joined_average):
    band_rows = make_band(kernel_taps, block_rows)
    row_width = band_rows.shape[2]
    if joined_average:
        band_rows = band_rows.reshape(2, block_rows // AVG, AVG, row_width).sum(axis=2) * (1.0 / AVG)
    out_count = band_rows.shape[1]
    stacked = band_rows.reshape(2 * out_count, row_width)
    product = jnp.dot(stacked, time_slab, precision=lax.Precision.HIGHEST, preferred_element_type=jnp.float32)
    prod_real = product[:out_count]
    prod_imag = product[out_count:]
    channels = time_slab.shape[1] // 2
    out_real = prod_real[:, :channels] - prod_imag[:, channels:]
    out_imag = prod_real[:, channels:] + prod_imag[:, :channels]
    result = jnp.stack([out_real, out_imag], axis=1)
    if not joined_average:
        result = result.reshape(out_count // AVG, AVG, 2, channels).sum(axis=1) * (1.0 / AVG)
    return result


def reference(visibilities, flag_mask, kernel_index, filter_bank):
    half_taps = TAPS // 2
    flag_float = flag_mask.astype(jnp.float32)
    taps_all = select_taps(kernel_index, filter_bank)
    block_count = TIMES // T_DEV

    def per_base(base_index):
        column = lax.dynamic_index_in_dim(visibilities, base_index, 1, False).astype(jnp.float32)
        column = (column * flag_float[:, None, None]).reshape(TIMES, 2 * CHAN)
        padded = jnp.pad(column, ((half_taps, half_taps), (0, 0)))
        kernel_taps = lax.dynamic_index_in_dim(taps_all, base_index, 0, False)

        def per_block(block_index):
            time_slab = lax.dynamic_slice_in_dim(padded, (block_index * T_DEV).astype(jnp.int32), T_DEV + TAPS - 1, 0)
            return filter_block(time_slab, kernel_taps, T_DEV, True)

        blocks_out = lax.map(per_block, jnp.arange(block_count, dtype=jnp.int32))
        return blocks_out.reshape(OUT_TIMES, 2, CHAN)

    filtered = lax.map(per_base, jnp.arange(BASE, dtype=jnp.int32))
    return jnp.moveaxis(filtered, 0, 1).astype(jnp.bfloat16)
```

```python
import functools

import jax
import jax.numpy as jnp
from jax import lax
from jax.experimental import pallas as pl
from jax.experimental.pallas import tpu as pltpu
from jax.sharding import PartitionSpec as P

AVG = 10
LANES = 1024
MESH = pl.DeviceIdType.MESH


def kernel(
    n, v_hbm, flag_ref, idx_ref, bank_ref, out_ref,
    vis, x0_ref, x1_ref, mask_ref, own, to_left, to_right, from_left, from_right, final,
    vis_sem, left_send, right_send, left_recv, right_recv, out_send, out_recv,
):
    bf16, f32 = jnp.bfloat16, jnp.float32
    me = lax.axis_index("tm")
    times, bases, _, chan = v_hbm.shape
    filters, taps = bank_ref.shape[1], bank_ref.shape[2]
    rows = times // AVG
    half = taps // 2
    over = to_left.shape[1]
    width = taps + AVG - 1
    every = rows + 2 * over
    groups = -(-2 * every // 8)

    barrier = pltpu.get_barrier_semaphore()
    for hop in range(1, n):
        pl.semaphore_signal(
            barrier, inc=1, device_id={"tm": lax.rem(me + hop, n)}, device_id_type=MESH
        )

    def base_at(step):
        middle = n // 2
        offset = middle + (1 - 2 * lax.rem(step, 2)) * ((step + 1) // 2)
        return lax.rem(me + offset, n)

    def fetch(base):
        return pltpu.make_async_copy(v_hbm.at[:, base], vis.at[base], vis_sem.at[base])

    def start_fetch(step, carry):
        fetch(base_at(step)).start()
        return carry

    lax.fori_loop(0, n, start_fetch, 0)

    @pl.when(me == 0)
    def _():
        from_left[...] = jnp.zeros_like(from_left)

    @pl.when(me == n - 1)
    def _():
        from_right[...] = jnp.zeros_like(from_right)

    lane = lax.broadcasted_iota(jnp.int32, (taps, LANES), 1)
    tap = lax.broadcasted_iota(jnp.int32, (taps, LANES), 0)
    base_shift = 2 * (AVG * over + half)
    offset = (((lane + base_shift) & (LANES - 1)) >> 1) - tap
    spread = jnp.where((offset >= 0) & (offset < AVG), 1.0, 0.0).astype(bf16)
    bank = jnp.concatenate([bank_ref[0], bank_ref[1]], axis=0)
    high = bank.astype(bf16)
    rest = bank - high.astype(f32)
    middle = rest.astype(bf16)
    low = (rest - middle.astype(f32)).astype(bf16)
    summed = (
        jnp.dot(high, spread, preferred_element_type=f32)
        + jnp.dot(middle, spread, preferred_element_type=f32)
        + jnp.dot(low, spread, preferred_element_type=f32)
    ) * (1.0 / AVG)
    even = (lax.broadcasted_iota(jnp.int32, (filters, LANES), 1) & 1) == 0
    x0_ref[...] = jnp.where(even, summed[:filters], -summed[filters:])
    x1_ref[...] = pltpu.roll(
        jnp.where(even, summed[filters:], summed[:filters]), LANES - AVG, 1
    )
    flags = flag_ref[...].reshape(1, times).astype(f32).astype(bf16)
    source = lax.broadcasted_iota(jnp.int32, (times, 2 * times), 0)
    target = lax.broadcasted_iota(jnp.int32, (times, 2 * times), 1)
    doubled = jnp.where((target >> 1) == source, 1.0, 0.0).astype(bf16)
    mask_ref[...] = jnp.dot(flags, doubled, preferred_element_type=f32)
    real_row = (lax.broadcasted_iota(jnp.int32, (8, LANES), 0) & 1) == 0

    def compute(step):
        base = base_at(step)
        which = idx_ref[base]
        x0 = jnp.broadcast_to(x0_ref[pl.ds(which, 1), :], (8, LANES))
        x1 = jnp.broadcast_to(x1_ref[pl.ds(which, 1), :], (8, LANES))
        eight = pltpu.roll(jnp.where(real_row, x0, x1), 0, 1, stride=AVG, stride_axis=0)
        band = jnp.concatenate(
            [pltpu.roll(eight, 8 * AVG * g, 1)[:, : 2 * times] for g in range(groups)], axis=0
        )
        band = band * mask_ref[...]
        band_high = band.astype(bf16)
        band_low = (band - band_high.astype(f32)).astype(bf16)
        fetch(base).wait()
        slab = vis[base].reshape(2 * times, chan)
        result = jnp.dot(band_high, slab, preferred_element_type=f32) + jnp.dot(
            band_low, slab, preferred_element_type=f32
        )
        to_left[base] = result[: 2 * over].reshape(over, 2, chan)
        own[base] = result[2 * over : 2 * (over + rows)]
        to_right[base] = result[2 * (over + rows) : 2 * every].reshape(over, 2, chan)

    def copy_left(base):
        return pltpu.make_async_remote_copy(
            src_ref=to_left.at[base], dst_ref=from_right.at[base],
            send_sem=left_send.at[base], recv_sem=right_recv.at[base],
            device_id={"tm": lax.rem(me + n - 1, n)}, device_id_type=MESH,
        )

    def copy_right(base):
        return pltpu.make_async_remote_copy(
            src_ref=to_right.at[base], dst_ref=from_left.at[base],
            send_sem=right_send.at[base], recv_sem=left_recv.at[base],
            device_id={"tm": lax.rem(me + 1, n)}, device_id_type=MESH,
        )

    def copy_out(base, source):
        return pltpu.make_async_remote_copy(
            src_ref=final.at[base], dst_ref=out_ref.at[pl.ds(source * rows, rows), 0],
            send_sem=out_send.at[base], recv_sem=out_recv.at[source],
            device_id={"tm": base}, device_id_type=MESH,
        )

    def copy_own():
        return pltpu.make_async_copy(
            final.at[me], out_ref.at[pl.ds(me * rows, rows), 0], out_send.at[me]
        )

    def send(step):
        base = base_at(step)

        @pl.when(me > 0)
        def _():
            copy_left(base).start()

        @pl.when(me < n - 1)
        def _():
            copy_right(base).start()

    compute(0)
    pl.semaphore_wait(barrier, n - 1)
    send(0)

    def first(step, carry):
        compute(step)
        send(step)
        return carry

    lax.fori_loop(1, n, first, 0)

    def second(step, carry):
        base = base_at(step)

        @pl.when(me > 0)
        def _():
            copy_right(base).wait_recv()

        @pl.when(me < n - 1)
        def _():
            copy_left(base).wait_recv()

        left = jnp.concatenate(
            [from_left[base].reshape(2 * over, chan), jnp.zeros((2 * (rows - over), chan), f32)], axis=0
        )
        right = jnp.concatenate(
            [jnp.zeros((2 * (rows - over), chan), f32), from_right[base].reshape(2 * over, chan)], axis=0
        )
        total = own[base] + left + right
        final[base] = total.astype(bf16).reshape(rows, 2, chan)

        @pl.when(base != me)
        def _():
            copy_out(base, me).start()

        @pl.when(base == me)
        def _():
            copy_own().start()

        return carry

    lax.fori_loop(0, n, second, 0)

    def finish(step, carry):
        base = base_at(step)

        @pl.when(me > 0)
        def _():
            copy_left(base).wait_send()

        @pl.when(me < n - 1)
        def _():
            copy_right(base).wait_send()

        @pl.when(base != me)
        def _():
            copy_out(base, base).wait_recv()
            copy_out(base, me).wait_send()

        @pl.when(base == me)
        def _():
            copy_own().wait()

        return carry

    lax.fori_loop(0, n, finish, 0)


def solution(mesh):
    n = mesh.shape["tm"]

    def per_device(visibilities, flag_mask, kernel_index, filter_bank):
        times, bases, _, chan = visibilities.shape
        _, filters, taps = filter_bank.shape
        rows = times // AVG
        over = -(-(taps // 2) // AVG)
        f32, bf16 = jnp.float32, jnp.bfloat16
        vmem = pl.BlockSpec(memory_space=pltpu.VMEM)
        hbm = pl.BlockSpec(memory_space=pl.ANY)
        dma = pltpu.SemaphoreType.DMA((bases,))
        return pl.pallas_call(
            functools.partial(kernel, n),
            out_shape=jax.ShapeDtypeStruct((n * rows, 1, 2, chan), bf16),
            in_specs=[hbm, vmem, pl.BlockSpec(memory_space=pltpu.SMEM), vmem],
            out_specs=hbm,
            scratch_shapes=[
                pltpu.VMEM((bases, times, 2, chan), bf16),
                pltpu.VMEM((filters, LANES), f32),
                pltpu.VMEM((filters, LANES), f32),
                pltpu.VMEM((1, 2 * times), f32),
                pltpu.VMEM((bases, 2 * rows, chan), f32),
                pltpu.VMEM((bases, over, 2, chan), f32),
                pltpu.VMEM((bases, over, 2, chan), f32),
                pltpu.VMEM((bases, over, 2, chan), f32),
                pltpu.VMEM((bases, over, 2, chan), f32),
                pltpu.VMEM((bases, rows, 2, chan), bf16),
                dma, dma, dma, dma, dma, dma, dma,
            ],
            compiler_params=pltpu.CompilerParams(
                collective_id=0, has_side_effects=True, vmem_limit_bytes=60 * 1024 * 1024
            ),
            name="fringe",
        )(visibilities, flag_mask, kernel_index, filter_bank)

    return jax.shard_map(
        per_device,
        mesh=mesh,
        in_specs=(
            P(("group", "tm"), ("bl", "pol"), None, None),
            P(("group", "tm")),
            P(("bl", "pol")),
            P(),
        ),
        out_specs=P("group", ("bl", "pol", "tm"), None, None),
        check_vma=False,
    )
```

```python
import functools

import jax
import jax.numpy as jnp
from jax import lax
from jax.experimental import pallas as pl
from jax.experimental.pallas import tpu as pltpu
from jax.sharding import PartitionSpec as P

AVG = 10
LANES = 1024
AHEAD = 5
LAST_LAG = 5
MESH = pl.DeviceIdType.MESH


def kernel(
    n, v_hbm, flag_ref, idx_ref, bank_ref, out_ref,
    vis, x0_ref, x1_ref, mask_ref, own, to_left, to_right, from_left, from_right, final,
    vis_sem, left_send, right_send, left_recv, right_recv, out_send, out_recv, ready,
):
    bf16, f32 = jnp.bfloat16, jnp.float32
    me = lax.axis_index("tm")
    times, bases, _, chan = v_hbm.shape
    filters, taps = bank_ref.shape[1], bank_ref.shape[2]
    rows = times // AVG
    half = taps // 2
    over = to_left.shape[1]
    width = taps + AVG - 1
    every = rows + 2 * over
    groups = -(-2 * every // 8)

    last = n - 1
    late = jnp.where(
        (lax.axis_index("group") == 0) & (lax.axis_index("bl") == 0) & (lax.axis_index("pol") == 0),
        1, 0,
    )

    def rank_of(place):
        return lax.rem(place + n - late, n)

    def at(rank):
        return lax.rem(rank + late, n)

    rank = rank_of(me)
    right_place, left_place = lax.rem(me + 1, n), lax.rem(me + last, n)
    has_left, has_right = me > 0, me < last
    left_waits = has_left & (rank_of(left_place) > rank)
    right_waits = has_right & (rank_of(right_place) > rank)

    def fetch(base):
        return pltpu.make_async_copy(v_hbm.at[:, base], vis.at[base], vis_sem.at[base])

    def start_fetch(step, carry):
        fetch(at(step)).start()
        return carry

    lax.fori_loop(0, bases, start_fetch, 0)

    barrier = pltpu.get_barrier_semaphore()

    @pl.when(rank > 0)
    def _():
        pl.semaphore_wait(barrier, 1)

    @pl.when(rank < last)
    def _():
        pl.semaphore_signal(
            barrier, inc=1, device_id={"tm": at(rank + 1)}, device_id_type=MESH
        )

    def announce(lower, carry):
        @pl.when(lower < rank)
        def _():
            pl.semaphore_signal(
                ready.at[me], inc=1, device_id={"tm": at(lower)}, device_id_type=MESH
            )

        return carry

    lax.fori_loop(0, last, announce, 0)

    @pl.when(me == 0)
    def _():
        from_left[...] = jnp.zeros_like(from_left)

    @pl.when(me == last)
    def _():
        from_right[...] = jnp.zeros_like(from_right)

    lane = lax.broadcasted_iota(jnp.int32, (taps, LANES), 1)
    tap = lax.broadcasted_iota(jnp.int32, (taps, LANES), 0)
    base_shift = 2 * (AVG * over + half)
    offset = (((lane + base_shift) & (LANES - 1)) >> 1) - tap
    spread = jnp.where((offset >= 0) & (offset < AVG), 1.0, 0.0).astype(bf16)
    bank = jnp.concatenate([bank_ref[0], bank_ref[1]], axis=0)
    high = bank.astype(bf16)
    rest = bank - high.astype(f32)
    middle = rest.astype(bf16)
    low = (rest - middle.astype(f32)).astype(bf16)
    summed = (
        jnp.dot(high, spread, preferred_element_type=f32)
        + jnp.dot(middle, spread, preferred_element_type=f32)
        + jnp.dot(low, spread, preferred_element_type=f32)
    ) * (1.0 / AVG)
    even = (lax.broadcasted_iota(jnp.int32, (filters, LANES), 1) & 1) == 0
    x0_ref[...] = jnp.where(even, summed[:filters], -summed[filters:])
    x1_ref[...] = pltpu.roll(
        jnp.where(even, summed[filters:], summed[:filters]), LANES - AVG, 1
    )
    flags = flag_ref[...].reshape(1, times).astype(f32).astype(bf16)
    source = lax.broadcasted_iota(jnp.int32, (times, 2 * times), 0)
    target = lax.broadcasted_iota(jnp.int32, (times, 2 * times), 1)
    doubled = jnp.where((target >> 1) == source, 1.0, 0.0).astype(bf16)
    mask_ref[...] = jnp.dot(flags, doubled, preferred_element_type=f32)
    real_row = (lax.broadcasted_iota(jnp.int32, (8, LANES), 0) & 1) == 0

    def compute(base):
        which = idx_ref[base]
        x0 = jnp.broadcast_to(x0_ref[pl.ds(which, 1), :], (8, LANES))
        x1 = jnp.broadcast_to(x1_ref[pl.ds(which, 1), :], (8, LANES))
        eight = pltpu.roll(jnp.where(real_row, x0, x1), 0, 1, stride=AVG, stride_axis=0)
        band = jnp.concatenate(
            [pltpu.roll(eight, 8 * AVG * g, 1)[:, : 2 * times] for g in range(groups)], axis=0
        )
        band = band * mask_ref[...]
        band_high = band.astype(bf16)
        band_low = (band - band_high.astype(f32)).astype(bf16)
        fetch(base).wait()
        slab = vis[base].reshape(2 * times, chan)
        result = jnp.dot(band_high, slab, preferred_element_type=f32) + jnp.dot(
            band_low, slab, preferred_element_type=f32
        )
        to_left[base] = result[: 2 * over].reshape(over, 2, chan)
        own[base] = result[2 * over : 2 * (over + rows)]
        to_right[base] = result[2 * (over + rows) : 2 * every].reshape(over, 2, chan)

    def copy_left(base):
        return pltpu.make_async_remote_copy(
            src_ref=to_left.at[base], dst_ref=from_right.at[base],
            send_sem=left_send.at[base], recv_sem=right_recv.at[base],
            device_id={"tm": lax.rem(me + n - 1, n)}, device_id_type=MESH,
        )

    def copy_right(base):
        return pltpu.make_async_remote_copy(
            src_ref=to_right.at[base], dst_ref=from_left.at[base],
            send_sem=right_send.at[base], recv_sem=left_recv.at[base],
            device_id={"tm": lax.rem(me + 1, n)}, device_id_type=MESH,
        )

    def copy_out(base, source):
        return pltpu.make_async_remote_copy(
            src_ref=final.at[base], dst_ref=out_ref.at[pl.ds(source * rows, rows), 0],
            send_sem=out_send.at[base], recv_sem=out_recv.at[source],
            device_id={"tm": base}, device_id_type=MESH,
        )

    def copy_own():
        return pltpu.make_async_copy(
            final.at[me], out_ref.at[pl.ds(me * rows, rows), 0], out_send.at[me]
        )

    def finish(step):
        base = at(step)

        @pl.when(has_left)
        def _():
            copy_right(base).wait_recv()

        @pl.when(has_right)
        def _():
            copy_left(base).wait_recv()

        pad = jnp.zeros((2 * (rows - over), chan), f32)
        left = jnp.concatenate([from_left[base].reshape(2 * over, chan), pad], axis=0)
        right = jnp.concatenate([pad, from_right[base].reshape(2 * over, chan)], axis=0)
        total = own[base] + left + right
        final[base] = total.astype(bf16).reshape(rows, 2, chan)

        met = (has_right & (base == right_place)) | (has_left & (base == left_place))

        @pl.when((step > rank) & jnp.logical_not(met))
        def _():
            pl.semaphore_wait(ready.at[base], 1)

        @pl.when(base != me)
        def _():
            copy_out(base, me).start()

        @pl.when(base == me)
        def _():
            copy_own().start()

        @pl.when(has_right & (step + AHEAD < bases))
        def _():
            copy_right(at(step + AHEAD)).start()

    soon = (me == last) | (rank == last)
    lag = jnp.where(soon, LAST_LAG, bases)

    def step_once(step, carry):
        @pl.when(step < bases)
        def _():
            compute(at(step))

            @pl.when(has_left & jnp.logical_not(left_waits))
            def _():
                copy_left(at(step)).start()

        @pl.when((step == AHEAD - 1) & right_waits)
        def _():
            pl.semaphore_wait(ready.at[right_place], 1)

        @pl.when((step == AHEAD - 1) & has_right)
        def _():
            for early in range(AHEAD):
                copy_right(at(early)).start()

        @pl.when((step == bases) & left_waits)
        def _():
            pl.semaphore_wait(ready.at[left_place], 1)

            def send_left(early, carry):
                copy_left(at(early)).start()
                return carry

            lax.fori_loop(0, bases, send_left, 0)

        @pl.when((step >= lag) & (step - lag < bases))
        def _():
            finish(step - lag)

        return carry

    lax.fori_loop(0, 2 * bases, step_once, 0)

    def drain(base, carry):
        @pl.when(has_left)
        def _():
            copy_left(base).wait_send()

        @pl.when(has_right)
        def _():
            copy_right(base).wait_send()

        @pl.when(base != me)
        def _():
            copy_out(base, base).wait_recv()
            copy_out(base, me).wait_send()

        @pl.when(base == me)
        def _():
            copy_own().wait()

        return carry

    lax.fori_loop(0, bases, drain, 0)


def solution(mesh):
    n = mesh.shape["tm"]

    def per_device(visibilities, flag_mask, kernel_index, filter_bank):
        times, bases, _, chan = visibilities.shape
        _, filters, taps = filter_bank.shape
        rows = times // AVG
        over = -(-(taps // 2) // AVG)
        f32, bf16 = jnp.float32, jnp.bfloat16
        vmem = pl.BlockSpec(memory_space=pltpu.VMEM)
        hbm = pl.BlockSpec(memory_space=pl.ANY)
        dma = pltpu.SemaphoreType.DMA((bases,))
        return pl.pallas_call(
            functools.partial(kernel, n),
            out_shape=jax.ShapeDtypeStruct((n * rows, 1, 2, chan), bf16),
            in_specs=[hbm, vmem, pl.BlockSpec(memory_space=pltpu.SMEM), vmem],
            out_specs=hbm,
            scratch_shapes=[
                pltpu.VMEM((bases, times, 2, chan), bf16),
                pltpu.VMEM((filters, LANES), f32),
                pltpu.VMEM((filters, LANES), f32),
                pltpu.VMEM((1, 2 * times), f32),
                pltpu.VMEM((bases, 2 * rows, chan), f32),
                pltpu.VMEM((bases, over, 2, chan), f32),
                pltpu.VMEM((bases, over, 2, chan), f32),
                pltpu.VMEM((bases, over, 2, chan), f32),
                pltpu.VMEM((bases, over, 2, chan), f32),
                pltpu.VMEM((bases, rows, 2, chan), bf16),
                dma, dma, dma, dma, dma, dma, dma,
                pltpu.SemaphoreType.REGULAR((n,)),
            ],
            compiler_params=pltpu.CompilerParams(
                collective_id=0, has_side_effects=True, vmem_limit_bytes=60 * 1024 * 1024
            ),
            name="fringe",
        )(visibilities, flag_mask, kernel_index, filter_bank)

    return jax.shard_map(
        per_device,
        mesh=mesh,
        in_specs=(
            P(("group", "tm"), ("bl", "pol"), None, None),
            P(("group", "tm")),
            P(("bl", "pol")),
            P(),
        ),
        out_specs=P("group", ("bl", "pol", "tm"), None, None),
        check_vma=False,
    )
```

```python
import functools

import jax
import jax.numpy as jnp
from jax import lax
from jax.experimental import pallas as pl
from jax.experimental.pallas import tpu as pltpu
from jax.sharding import PartitionSpec as P

AVG = 10
LANES = 1024
PAIR = 4
AHEAD = 4
EARLY = 1
MESH = pl.DeviceIdType.MESH


def kernel(
    n, v_hbm, flag_ref, idx_ref, bank_ref, out_ref,
    vis, x0_ref, x1_ref, mask_ref, own, to_left, to_right, from_left, from_right, final,
    vis_sem, left_send, right_send, left_recv, right_recv, out_send, out_recv, ready,
):
    bf16, f32 = jnp.bfloat16, jnp.float32
    me = lax.axis_index("tm")
    times, bases, _, chan = v_hbm.shape
    filters, taps = bank_ref.shape[1], bank_ref.shape[2]
    rows = times // AVG
    half = taps // 2
    over = to_left.shape[1]
    width = taps + AVG - 1
    every = rows + 2 * over
    groups = -(-2 * every // 8)

    last = n - 1
    late = jnp.where(
        (lax.axis_index("group") == 0) & (lax.axis_index("bl") == 0) & (lax.axis_index("pol") == 0),
        1, 0,
    )

    def rank_of(place):
        return lax.rem(place + n - late, n)

    def at(rank):
        return lax.rem(rank + late, n)

    rank = rank_of(me)
    right_place, left_place = lax.rem(me + 1, n), lax.rem(me + last, n)
    has_left, has_right = me > 0, me < last
    left_waits = has_left & (rank_of(left_place) > rank)
    right_waits = has_right & (rank_of(right_place) > rank)

    def fetch(base):
        return pltpu.make_async_copy(v_hbm.at[:, base], vis.at[base], vis_sem.at[base])

    def start_fetch(step, carry):
        fetch(at(step)).start()
        return carry

    lax.fori_loop(0, bases, start_fetch, 0)

    barrier = pltpu.get_barrier_semaphore()

    @pl.when(rank > 0)
    def _():
        pl.semaphore_wait(barrier, 1)

    @pl.when(rank < last)
    def _():
        pl.semaphore_signal(
            barrier, inc=1, device_id={"tm": at(rank + 1)}, device_id_type=MESH
        )

    def announce(lower, carry):
        @pl.when(lower < rank)
        def _():
            pl.semaphore_signal(
                ready.at[me], inc=1, device_id={"tm": at(lower)}, device_id_type=MESH
            )

        return carry

    lax.fori_loop(0, last, announce, 0)

    @pl.when(me == 0)
    def _():
        from_left[...] = jnp.zeros_like(from_left)

    @pl.when(me == last)
    def _():
        from_right[...] = jnp.zeros_like(from_right)

    lane = lax.broadcasted_iota(jnp.int32, (taps, LANES), 1)
    tap = lax.broadcasted_iota(jnp.int32, (taps, LANES), 0)
    base_shift = 2 * (AVG * over + half)
    offset = (((lane + base_shift) & (LANES - 1)) >> 1) - tap
    spread = jnp.where((offset >= 0) & (offset < AVG), 1.0, 0.0).astype(bf16)
    bank = jnp.concatenate([bank_ref[0], bank_ref[1]], axis=0)
    high = bank.astype(bf16)
    rest = bank - high.astype(f32)
    middle = rest.astype(bf16)
    low = (rest - middle.astype(f32)).astype(bf16)
    summed = (
        jnp.dot(high, spread, preferred_element_type=f32)
        + jnp.dot(middle, spread, preferred_element_type=f32)
        + jnp.dot(low, spread, preferred_element_type=f32)
    ) * (1.0 / AVG)
    even = (lax.broadcasted_iota(jnp.int32, (filters, LANES), 1) & 1) == 0
    x0_ref[...] = jnp.where(even, summed[:filters], -summed[filters:])
    x1_ref[...] = pltpu.roll(
        jnp.where(even, summed[filters:], summed[:filters]), LANES - AVG, 1
    )
    flags = flag_ref[...].reshape(1, times).astype(f32).astype(bf16)
    source = lax.broadcasted_iota(jnp.int32, (times, 2 * times), 0)
    target = lax.broadcasted_iota(jnp.int32, (times, 2 * times), 1)
    doubled = jnp.where((target >> 1) == source, 1.0, 0.0).astype(bf16)
    mask_ref[...] = jnp.dot(flags, doubled, preferred_element_type=f32)
    real_row = (lax.broadcasted_iota(jnp.int32, (8, LANES), 0) & 1) == 0

    def compute(base):
        which = idx_ref[base]
        x0 = jnp.broadcast_to(x0_ref[pl.ds(which, 1), :], (8, LANES))
        x1 = jnp.broadcast_to(x1_ref[pl.ds(which, 1), :], (8, LANES))
        eight = pltpu.roll(jnp.where(real_row, x0, x1), 0, 1, stride=AVG, stride_axis=0)
        band = jnp.concatenate(
            [pltpu.roll(eight, 8 * AVG * g, 1)[:, : 2 * times] for g in range(groups)], axis=0
        )
        band = band * mask_ref[...]
        band_high = band.astype(bf16)
        band_low = (band - band_high.astype(f32)).astype(bf16)
        fetch(base).wait()
        slab = vis[base].reshape(2 * times, chan)
        result = jnp.dot(band_high, slab, preferred_element_type=f32) + jnp.dot(
            band_low, slab, preferred_element_type=f32
        )
        to_left[base] = result[: 2 * over].reshape(over, 2, chan)
        own[base] = result[2 * over : 2 * (over + rows)]
        to_right[base] = result[2 * (over + rows) : 2 * every].reshape(over, 2, chan)

    def copy_left(base):
        return pltpu.make_async_remote_copy(
            src_ref=to_left.at[base], dst_ref=from_right.at[base],
            send_sem=left_send.at[base], recv_sem=right_recv.at[base],
            device_id={"tm": lax.rem(me + n - 1, n)}, device_id_type=MESH,
        )

    def copy_right(base):
        return pltpu.make_async_remote_copy(
            src_ref=to_right.at[base], dst_ref=from_left.at[base],
            send_sem=right_send.at[base], recv_sem=left_recv.at[base],
            device_id={"tm": lax.rem(me + 1, n)}, device_id_type=MESH,
        )

    def copy_out(base, source):
        return pltpu.make_async_remote_copy(
            src_ref=final.at[base], dst_ref=out_ref.at[pl.ds(source * rows, rows), 0],
            send_sem=out_send.at[base], recv_sem=out_recv.at[source],
            device_id={"tm": base}, device_id_type=MESH,
        )

    def copy_own():
        return pltpu.make_async_copy(
            final.at[me], out_ref.at[pl.ds(me * rows, rows), 0], out_send.at[me]
        )

    paced = me >= n // 2

    def finish(step):
        base = at(step)

        @pl.when(has_left)
        def _():
            copy_right(base).wait_recv()

        @pl.when(has_right)
        def _():
            copy_left(base).wait_recv()

        pad = jnp.zeros((2 * (rows - over), chan), f32)
        left = jnp.concatenate([from_left[base].reshape(2 * over, chan), pad], axis=0)
        right = jnp.concatenate([pad, from_right[base].reshape(2 * over, chan)], axis=0)
        total = own[base] + left + right
        final[base] = total.astype(bf16).reshape(rows, 2, chan)

        met = (has_right & (base == right_place)) | (has_left & (base == left_place))

        @pl.when((step > rank) & jnp.logical_not(met))
        def _():
            pl.semaphore_wait(ready.at[base], 1)

        @pl.when(base != me)
        def _():
            copy_out(base, me).start()

        @pl.when(base == me)
        def _():
            copy_own().start()

        @pl.when(paced & has_right & (step + AHEAD < bases))
        def _():
            copy_right(at(step + AHEAD)).start()

    soon = me == last
    steps = bases // PAIR
    lag = jnp.where(soon, EARLY, jnp.where(paced, 2, steps))

    def step_once(step, carry):
        @pl.when(step < steps)
        def _():
            for part in range(PAIR):
                compute(at(step * PAIR + part))

            @pl.when(has_left & jnp.logical_not(left_waits))
            def _():
                for part in range(PAIR):
                    copy_left(at(step * PAIR + part)).start()

        @pl.when((step == AHEAD // PAIR - 1) & right_waits)
        def _():
            pl.semaphore_wait(ready.at[right_place], 1)

        @pl.when((step == AHEAD // PAIR - 1) & has_right)
        def _():
            for early in range(AHEAD):
                copy_right(at(early)).start()

        @pl.when((step >= AHEAD // PAIR) & (step < steps) & has_right & jnp.logical_not(paced))
        def _():
            for part in range(PAIR):
                copy_right(at(step * PAIR + part)).start()

        @pl.when((step == steps) & left_waits)
        def _():
            pl.semaphore_wait(ready.at[left_place], 1)

            def send_left(early, carry):
                copy_left(at(early)).start()
                return carry

            lax.fori_loop(0, bases, send_left, 0)

        @pl.when((step >= lag) & (step < lag + steps))
        def _():
            def second(part, carry):
                finish((step - lag) * PAIR + part)
                return carry

            lax.fori_loop(0, PAIR, second, 0)

        return carry

    lax.fori_loop(0, lag + steps, step_once, 0)

    def drain(base, carry):
        @pl.when(has_left)
        def _():
            copy_left(base).wait_send()

        @pl.when(has_right)
        def _():
            copy_right(base).wait_send()

        @pl.when(base != me)
        def _():
            copy_out(base, base).wait_recv()
            copy_out(base, me).wait_send()

        @pl.when(base == me)
        def _():
            copy_own().wait()

        return carry

    lax.fori_loop(0, bases, drain, 0)


def solution(mesh):
    n = mesh.shape["tm"]

    def per_device(visibilities, flag_mask, kernel_index, filter_bank):
        times, bases, _, chan = visibilities.shape
        _, filters, taps = filter_bank.shape
        rows = times // AVG
        over = -(-(taps // 2) // AVG)
        f32, bf16 = jnp.float32, jnp.bfloat16
        vmem = pl.BlockSpec(memory_space=pltpu.VMEM)
        hbm = pl.BlockSpec(memory_space=pl.ANY)
        dma = pltpu.SemaphoreType.DMA((bases,))
        return pl.pallas_call(
            functools.partial(kernel, n),
            out_shape=jax.ShapeDtypeStruct((n * rows, 1, 2, chan), bf16),
            in_specs=[hbm, vmem, pl.BlockSpec(memory_space=pltpu.SMEM), vmem],
            out_specs=hbm,
            scratch_shapes=[
                pltpu.VMEM((bases, times, 2, chan), bf16),
                pltpu.VMEM((filters, LANES), f32),
                pltpu.VMEM((filters, LANES), f32),
                pltpu.VMEM((1, 2 * times), f32),
                pltpu.VMEM((bases, 2 * rows, chan), f32),
                pltpu.VMEM((bases, over, 2, chan), f32),
                pltpu.VMEM((bases, over, 2, chan), f32),
                pltpu.VMEM((bases, over, 2, chan), f32),
                pltpu.VMEM((bases, over, 2, chan), f32),
                pltpu.VMEM((bases, rows, 2, chan), bf16),
                dma, dma, dma, dma, dma, dma, dma,
                pltpu.SemaphoreType.REGULAR((n,)),
            ],
            compiler_params=pltpu.CompilerParams(
                collective_id=0, has_side_effects=True, vmem_limit_bytes=60 * 1024 * 1024
            ),
            name="fringe",
        )(visibilities, flag_mask, kernel_index, filter_bank)

    return jax.shard_map(
        per_device,
        mesh=mesh,
        in_specs=(
            P(("group", "tm"), ("bl", "pol"), None, None),
            P(("group", "tm")),
            P(("bl", "pol")),
            P(),
        ),
        out_specs=P("group", ("bl", "pol", "tm"), None, None),
        check_vma=False,
    )
```

```python
import functools

import jax
import jax.numpy as jnp
from jax import lax
from jax.experimental import pallas as pl
from jax.experimental.pallas import tpu as pltpu
from jax.sharding import PartitionSpec as P

AVG = 10
LANES = 1024
PAIR = 4
AHEAD = 4
EARLY = 1
MESH = pl.DeviceIdType.MESH


def kernel(
    n, v_hbm, flag_ref, idx_ref, bank_ref, out_ref,
    vis, x0_ref, x1_ref, mask_ref, own, to_left, to_right, from_left, from_right, final,
    vis_sem, left_send, right_send, left_recv, right_recv, out_send, out_recv, ready,
):
    bf16, f32 = jnp.bfloat16, jnp.float32
    me = lax.axis_index("tm")
    times, bases, _, chan = v_hbm.shape
    filters, taps = bank_ref.shape[1], bank_ref.shape[2]
    rows = times // AVG
    half = taps // 2
    over = to_left.shape[1]
    width = taps + AVG - 1
    every = rows + 2 * over
    groups = -(-2 * every // 8)

    last = n - 1
    late = jnp.where(
        (lax.axis_index("group") == 0) & (lax.axis_index("bl") == 0) & (lax.axis_index("pol") == 0),
        1, 0,
    )

    def rank_of(place):
        return lax.rem(place + n - late, n)

    def at(rank):
        return lax.rem(rank + late, n)

    rank = rank_of(me)
    right_place, left_place = lax.rem(me + 1, n), lax.rem(me + last, n)
    has_left, has_right = me > 0, me < last
    left_waits = has_left & (rank_of(left_place) > rank)
    right_waits = has_right & (rank_of(right_place) > rank)

    def fetch(base):
        return pltpu.make_async_copy(v_hbm.at[:, base], vis.at[base], vis_sem.at[base])

    def start_fetch(step, carry):
        fetch(at(step)).start()
        return carry

    lax.fori_loop(0, bases, start_fetch, 0)

    barrier = pltpu.get_barrier_semaphore()

    def enter():
        @pl.when(rank > 0)
        def _():
            pl.semaphore_wait(barrier, 1)

        @pl.when(rank < last)
        def _():
            pl.semaphore_signal(
                barrier, inc=1, device_id={"tm": at(rank + 1)}, device_id_type=MESH
            )

        def announce(lower, carry):
            @pl.when(lower < rank)
            def _():
                pl.semaphore_signal(
                    ready.at[me], inc=1, device_id={"tm": at(lower)}, device_id_type=MESH
                )

            return carry

        lax.fori_loop(0, last, announce, 0)

    enter_late = (late == 1) & (rank == last)

    @pl.when(jnp.logical_not(enter_late))
    def _():
        enter()

    @pl.when(me == 0)
    def _():
        from_left[...] = jnp.zeros_like(from_left)

    @pl.when(me == last)
    def _():
        from_right[...] = jnp.zeros_like(from_right)

    lane = lax.broadcasted_iota(jnp.int32, (taps, LANES), 1)
    tap = lax.broadcasted_iota(jnp.int32, (taps, LANES), 0)
    base_shift = 2 * (AVG * over + half)
    offset = (((lane + base_shift) & (LANES - 1)) >> 1) - tap
    spread = jnp.where((offset >= 0) & (offset < AVG), 1.0, 0.0).astype(bf16)
    bank = jnp.concatenate([bank_ref[0], bank_ref[1]], axis=0)
    high = bank.astype(bf16)
    rest = bank - high.astype(f32)
    middle = rest.astype(bf16)
    low = (rest - middle.astype(f32)).astype(bf16)
    summed = (
        jnp.dot(high, spread, preferred_element_type=f32)
        + jnp.dot(middle, spread, preferred_element_type=f32)
        + jnp.dot(low, spread, preferred_element_type=f32)
    ) * (1.0 / AVG)
    even = (lax.broadcasted_iota(jnp.int32, (filters, LANES), 1) & 1) == 0
    x0_ref[...] = jnp.where(even, summed[:filters], -summed[filters:])
    x1_ref[...] = pltpu.roll(
        jnp.where(even, summed[filters:], summed[:filters]), LANES - AVG, 1
    )
    flags = flag_ref[...].reshape(1, times).astype(f32).astype(bf16)
    source = lax.broadcasted_iota(jnp.int32, (times, 2 * times), 0)
    target = lax.broadcasted_iota(jnp.int32, (times, 2 * times), 1)
    doubled = jnp.where((target >> 1) == source, 1.0, 0.0).astype(bf16)
    mask_ref[...] = jnp.dot(flags, doubled, preferred_element_type=f32)
    real_row = (lax.broadcasted_iota(jnp.int32, (8, LANES), 0) & 1) == 0

    def compute(base):
        which = idx_ref[base]
        x0 = jnp.broadcast_to(x0_ref[pl.ds(which, 1), :], (8, LANES))
        x1 = jnp.broadcast_to(x1_ref[pl.ds(which, 1), :], (8, LANES))
        eight = pltpu.roll(jnp.where(real_row, x0, x1), 0, 1, stride=AVG, stride_axis=0)
        band = jnp.concatenate(
            [pltpu.roll(eight, 8 * AVG * g, 1)[:, : 2 * times] for g in range(groups)], axis=0
        )
        band = band * mask_ref[...]
        band_high = band.astype(bf16)
        band_low = (band - band_high.astype(f32)).astype(bf16)
        fetch(base).wait()
        slab = vis[base].reshape(2 * times, chan)
        result = jnp.dot(band_high, slab, preferred_element_type=f32) + jnp.dot(
            band_low, slab, preferred_element_type=f32
        )
        to_left[base] = result[: 2 * over].reshape(over, 2, chan)
        own[base] = result[2 * over : 2 * (over + rows)]
        to_right[base] = result[2 * (over + rows) : 2 * every].reshape(over, 2, chan)

    def copy_left(base):
        return pltpu.make_async_remote_copy(
            src_ref=to_left.at[base], dst_ref=from_right.at[base],
            send_sem=left_send.at[base], recv_sem=right_recv.at[base],
            device_id={"tm": lax.rem(me + n - 1, n)}, device_id_type=MESH,
        )

    def copy_right(base):
        return pltpu.make_async_remote_copy(
            src_ref=to_right.at[base], dst_ref=from_left.at[base],
            send_sem=right_send.at[base], recv_sem=left_recv.at[base],
            device_id={"tm": lax.rem(me + 1, n)}, device_id_type=MESH,
        )

    def copy_out(base, source):
        return pltpu.make_async_remote_copy(
            src_ref=final.at[base], dst_ref=out_ref.at[pl.ds(source * rows, rows), 0],
            send_sem=out_send.at[base], recv_sem=out_recv.at[source],
            device_id={"tm": base}, device_id_type=MESH,
        )

    def copy_own():
        return pltpu.make_async_copy(
            final.at[me], out_ref.at[pl.ds(me * rows, rows), 0], out_send.at[me]
        )

    paced = me >= n // 2

    def finish(step):
        base = at(step)

        @pl.when(has_left)
        def _():
            copy_right(base).wait_recv()

        @pl.when(has_right)
        def _():
            copy_left(base).wait_recv()

        pad = jnp.zeros((2 * (rows - over), chan), f32)
        left = jnp.concatenate([from_left[base].reshape(2 * over, chan), pad], axis=0)
        right = jnp.concatenate([pad, from_right[base].reshape(2 * over, chan)], axis=0)
        total = own[base] + left + right
        final[base] = total.astype(bf16).reshape(rows, 2, chan)

        met = (has_right & (base == right_place)) | (has_left & (base == left_place))

        @pl.when((step > rank) & jnp.logical_not(met))
        def _():
            pl.semaphore_wait(ready.at[base], 1)

        @pl.when(base != me)
        def _():
            copy_out(base, me).start()

        @pl.when(base == me)
        def _():
            copy_own().start()

        @pl.when(paced & has_right & (step + AHEAD < bases))
        def _():
            copy_right(at(step + AHEAD)).start()

    soon = me == last
    steps = bases // PAIR
    lag = jnp.where(soon, EARLY, jnp.where(paced, 2, steps))

    def step_once(step, carry):
        @pl.when(step < steps)
        def _():
            for part in range(PAIR):
                compute(at(step * PAIR + part))

            @pl.when((step == 0) & enter_late)
            def _():
                enter()

            @pl.when(has_left & jnp.logical_not(left_waits))
            def _():
                for part in range(PAIR):
                    copy_left(at(step * PAIR + part)).start()

        @pl.when((step == AHEAD // PAIR - 1) & right_waits)
        def _():
            pl.semaphore_wait(ready.at[right_place], 1)

        @pl.when((step == AHEAD // PAIR - 1) & has_right)
        def _():
            for early in range(AHEAD):
                copy_right(at(early)).start()

        @pl.when((step >= AHEAD // PAIR) & (step < steps) & has_right & jnp.logical_not(paced))
        def _():
            for part in range(PAIR):
                copy_right(at(step * PAIR + part)).start()

        @pl.when((step == steps) & left_waits)
        def _():
            pl.semaphore_wait(ready.at[left_place], 1)

            def send_left(early, carry):
                copy_left(at(early)).start()
                return carry

            lax.fori_loop(0, bases, send_left, 0)

        @pl.when((step >= lag) & (step < lag + steps))
        def _():
            def second(part, carry):
                finish((step - lag) * PAIR + part)
                return carry

            lax.fori_loop(0, PAIR, second, 0)

        return carry

    lax.fori_loop(0, lag + steps, step_once, 0)

    def drain(base, carry):
        @pl.when(has_left)
        def _():
            copy_left(base).wait_send()

        @pl.when(has_right)
        def _():
            copy_right(base).wait_send()

        @pl.when(base != me)
        def _():
            copy_out(base, base).wait_recv()
            copy_out(base, me).wait_send()

        @pl.when(base == me)
        def _():
            copy_own().wait()

        return carry

    lax.fori_loop(0, bases, drain, 0)


def solution(mesh):
    n = mesh.shape["tm"]

    def per_device(visibilities, flag_mask, kernel_index, filter_bank):
        times, bases, _, chan = visibilities.shape
        _, filters, taps = filter_bank.shape
        rows = times // AVG
        over = -(-(taps // 2) // AVG)
        f32, bf16 = jnp.float32, jnp.bfloat16
        vmem = pl.BlockSpec(memory_space=pltpu.VMEM)
        hbm = pl.BlockSpec(memory_space=pl.ANY)
        dma = pltpu.SemaphoreType.DMA((bases,))
        return pl.pallas_call(
            functools.partial(kernel, n),
            out_shape=jax.ShapeDtypeStruct((n * rows, 1, 2, chan), bf16),
            in_specs=[hbm, vmem, pl.BlockSpec(memory_space=pltpu.SMEM), vmem],
            out_specs=hbm,
            scratch_shapes=[
                pltpu.VMEM((bases, times, 2, chan), bf16),
                pltpu.VMEM((filters, LANES), f32),
                pltpu.VMEM((filters, LANES), f32),
                pltpu.VMEM((1, 2 * times), f32),
                pltpu.VMEM((bases, 2 * rows, chan), f32),
                pltpu.VMEM((bases, over, 2, chan), f32),
                pltpu.VMEM((bases, over, 2, chan), f32),
                pltpu.VMEM((bases, over, 2, chan), f32),
                pltpu.VMEM((bases, over, 2, chan), f32),
                pltpu.VMEM((bases, rows, 2, chan), bf16),
                dma, dma, dma, dma, dma, dma, dma,
                pltpu.SemaphoreType.REGULAR((n,)),
            ],
            compiler_params=pltpu.CompilerParams(
                collective_id=0, has_side_effects=True, vmem_limit_bytes=60 * 1024 * 1024
            ),
            name="fringe",
        )(visibilities, flag_mask, kernel_index, filter_bank)

    return jax.shard_map(
        per_device,
        mesh=mesh,
        in_specs=(
            P(("group", "tm"), ("bl", "pol"), None, None),
            P(("group", "tm")),
            P(("bl", "pol")),
            P(),
        ),
        out_specs=P("group", ("bl", "pol", "tm"), None, None),
        check_vma=False,
    )
```
